32 devices in a mesh: seq: 8 (over y, x, core), head: 4 (over z).
Axes of the slice: x: 2, y: 2, z: 4, core: 2. Of those that a mesh axis runs over, the one named last changes fastest.
Arguments:
- segment_input: bfloat16 [2, 2048, 3584], P(None, 'seq'), may hold values from -16 to 16
- doc_ids: int32 [2, 2048], replicated, may hold values from 0 to 3, never falling along the last dimension, each value on 1 to 1024 neighbouring positions
- memory: bfloat16 [32, 3584], replicated, may hold values from -16 to 16
- gain: bfloat16 [3584], replicated, may hold values from 0.099609375 to 1.8984375
- w_query: bfloat16 [3584, 4096], P(None, 'head'), may hold values from -4 to 4
- w_key: bfloat16 [3584, 2048], P(None, 'head'), may hold values from -4 to 4
- w_value: bfloat16 [3584, 2048], P(None, 'head'), may hold values from -0.09375 to 0.09375
- w_out: bfloat16 [4096, 3584], P(None, 'head'), may hold values from -0.09375 to 0.09375
- mem_proj: bfloat16 [3584, 3584], P('head'), may hold values from -4 to 4
Outputs:
- hidden: bfloat16 [2, 2048, 3584], P(None, 'seq', 'head')
- new_memory: bfloat16 [32, 3584], replicated
The draws below stay inside these ranges and needn't reach their ends.
Inputs may be any that keep to these rules, and one draw needn't show every extreme that they name: `doc_ids`: ids never fall along a segment; each document has 1 to 1024 tokens.
All inputs are finite; a program needn't handle non-finite values.
Results may differ from the reference program's by a relative error of at most 0.02.
Values may be sent and summed in bfloat16 or wider, within the bound.
A program may use at most 128 MiB of HBM per device.

```python
import math
import jax
import jax.numpy as jnp
import numpy as np
from jax import lax

D = 3584
HEADS = 16
KV_HEADS = 8
HD = 256
M = 32
SEGS = 2
TOKENS = 2048


def drawn_rows(row_key, row_count):
    return jnp.clip(jax.random.normal(jax.random.fold_in(row_key, 1), (row_count, D), jnp.float32), -6.0, 6.0)


def draw_segment_input(key, part):
    pieces = []
    for segment in range(SEGS):
        row_key = jax.random.fold_in(key, 500 + segment)
        pieces.append(drawn_rows(row_key, TOKENS))
    return jnp.stack(pieces, axis=0).astype(jnp.bfloat16)


def draw_memory(key, part):
    row_key = jax.random.fold_in(key, 700)
    result = drawn_rows(row_key, M)
    return result.astype(jnp.bfloat16)


def draw_w_query(key, part):
    weights = jnp.clip(jax.random.normal(jax.random.fold_in(key, 9201), (D, HEADS, HD), jnp.float32), -4.0, 4.0) * D ** (-0.5)
    return weights.reshape(D, HEADS * HD).astype(jnp.bfloat16)


def draw_w_key(key, part):
    weights = jnp.clip(jax.random.normal(jax.random.fold_in(key, 9202), (D, KV_HEADS, HD), jnp.float32), -4.0, 4.0) * D ** (-0.5)
    return weights.reshape(D, KV_HEADS * HD).astype(jnp.bfloat16)


def draw_mem_proj(key, part):
    weights = jnp.clip(jax.random.normal(jax.random.fold_in(key, 9203), (D, D), jnp.float32), -4.0, 4.0) * D ** (-0.5)
    return weights.astype(jnp.bfloat16)


def steps_of(own_key, dims, split, smallest, high):
    def one(dim, parts):
        steps = jax.random.uniform(jax.random.fold_in(jax.random.fold_in(own_key, 6), dim), (parts,), jnp.float32, smallest / len(split), high / len(split))
        return jnp.repeat(jnp.exp(steps), dims[dim] // parts).reshape((-1,) + (1,) * (len(dims) - dim - 1))

    loudness = one(*split[0])
    for cut in split[1:]:
        loudness = loudness * one(*cut)
    return loudness


def split_up(number_of, total, bound, lean):
    weights = [(1 << 20) // math.isqrt(rank ** lean) + 1 for rank in range(2, number_of + 1)]
    rest, counts = total - bound - (number_of - 1), [1] * (number_of - 1)
    while rest > 0:
        candidates = [i for i in range(number_of - 1) if counts[i] < bound]
        pool, budget = sum([weights[i] for i in candidates]), rest
        for i in candidates:
            extra = min(bound - counts[i], max(1, budget * weights[i] // pool), rest)
            counts[i] = counts[i] + extra
            rest = rest - extra
    return np.array([bound] + counts)


def ragged_sizes(rng, amount, total, most, slope):
    if amount == 2:
        one = jax.random.randint(rng, (), max(1, total - most), min(most, total - 1) + 1)
        return jnp.stack([one, total - one])
    sizes = jnp.asarray(split_up(amount, total, most, slope), jnp.int32)
    twos = (amount - 1) // 2
    source_of, taker = sizes[1:1 + 2 * twos:2], sizes[2:2 + 2 * twos:2]
    room = jnp.minimum(source_of - 1, most - taker)
    moved = jax.random.randint(jax.random.fold_in(rng, 1), (twos,), 0, 1 << 20) % (room + 1)
    sizes = sizes.at[1:1 + 2 * twos:2].set(source_of - moved).at[2:2 + 2 * twos:2].set(taker + moved)
    return sizes[jax.random.permutation(jax.random.fold_in(rng, 2), amount)]


def normal_values(own_key, extent, spread, limit, cuts=(), held_as=jnp.bfloat16):
    values = jax.random.normal(own_key, extent, jnp.float32) * spread
    if len(cuts) > 0:
        values = steps_of(own_key, extent, cuts, -0.22, 0.18) * values
    return jnp.clip(values, min=-limit, max=limit).astype(held_as)


def setup_inputs(seed: int = 0) -> dict:
    splits = jax.random.split(jax.random.key(seed), 10)
    return {
        "segment_input": draw_segment_input(jax.random.fold_in(splits[9], 71), 0),
        "doc_ids": jax.vmap(lambda own: jnp.searchsorted(jnp.cumsum(ragged_sizes(own, 4, TOKENS, TOKENS // 2, 0)), jnp.arange(TOKENS), side="right"))(jax.random.split(splits[1], SEGS)).reshape((SEGS, TOKENS)).astype(jnp.int32),
        "memory": draw_memory(jax.random.fold_in(splits[9], 71), 0),
        "gain": jnp.clip(1.0 + 0.18 * jax.random.normal(splits[3], (D,), jnp.float32), 0.099609375, 1.8984375).astype(jnp.bfloat16),
        "w_query": draw_w_query(jax.random.fold_in(splits[9], 71), 0),
        "w_key": draw_w_key(jax.random.fold_in(splits[9], 71), 0),
        "w_value": normal_values(splits[6], (D, KV_HEADS * HD), D ** -0.5, 0.09375, ((1, 4),)),
        "w_out": normal_values(splits[7], (HEADS * HD, D), (HEADS * HD) ** -0.5, 0.09375, ((1, 4),)),
        "mem_proj": draw_mem_proj(jax.random.fold_in(splits[9], 71), 0),
    }


def rms_norm(rows, gain):
    values = rows.astype(jnp.float32)
    scaled = values * lax.rsqrt(lax.optimization_barrier(jnp.mean(values * values, axis=-1, keepdims=True)) + 1e-06)
    return (scaled * gain.astype(jnp.float32)).astype(jnp.bfloat16)

def reference(segment_input, doc_ids, memory, gain, w_query, w_key, w_value, w_out, mem_proj):
    mem = memory
    outputs = []
    scale = jnp.float32(HD ** (-0.5))
    for seg in range(SEGS):
        tokens = segment_input[seg]
        docs = doc_ids[seg]
        normed_x = rms_norm(tokens, gain)
        normed_m = rms_norm(mem, gain)
        rows_all = jnp.concatenate([normed_x, normed_m], axis=0)
        query = jnp.dot(rows_all, w_query, preferred_element_type=jnp.float32).astype(jnp.bfloat16)
        keys = jnp.dot(rows_all, w_key, preferred_element_type=jnp.float32).astype(jnp.bfloat16)
        values = jnp.dot(rows_all, w_value, preferred_element_type=jnp.float32).astype(jnp.bfloat16)
        rows = TOKENS + M
        query = query.reshape(rows, KV_HEADS, 2, HD).transpose(1, 0, 2, 3)
        keys = jnp.concatenate([keys[TOKENS:], keys[:TOKENS]], axis=0).reshape(rows, KV_HEADS, HD).transpose(1, 0, 2)
        values = jnp.concatenate([values[TOKENS:], values[:TOKENS]], axis=0).reshape(rows, KV_HEADS, HD).transpose(1, 0, 2)
        position = jnp.arange(TOKENS, dtype=jnp.int32)
        allowed = (position[None, :] <= position[:, None]) & (docs[None, :] == docs[:, None])
        token_mask = jnp.concatenate([jnp.ones((TOKENS, M), dtype=bool), allowed], axis=1)
        mask = jnp.concatenate([token_mask, jnp.ones((M, rows), dtype=bool)], axis=0)

        def one_group(operands):
            group_query, group_keys, group_values = operands
            scores = jnp.einsum('rgd,kd->grk', group_query.astype(jnp.float32), group_keys.astype(jnp.float32)) * scale
            scores = jnp.where(mask[None], scores, -1e+30)
            peak = lax.optimization_barrier(jnp.max(scores, axis=-1, keepdims=True))
            weights = jnp.where(mask[None], jnp.exp(scores - peak), 0.0)
            total = lax.optimization_barrier(jnp.sum(weights, axis=-1))
            mixed = jnp.einsum('grk,kd->grd', weights.astype(jnp.bfloat16).astype(jnp.float32), group_values.astype(jnp.float32))
            return mixed / total[..., None]
        attended = lax.map(one_group, (query, keys, values))
        attended = attended.transpose(2, 0, 1, 3).reshape(rows, HEADS * HD).astype(jnp.bfloat16)
        attn_tok = attended[:TOKENS]
        attn_mem = attended[TOKENS:]
        outputs.append((tokens.astype(jnp.float32) + jnp.dot(attn_tok, w_out, preferred_element_type=jnp.float32)).astype(jnp.bfloat16))
        mem_out = (mem.astype(jnp.float32) + jnp.dot(attn_mem, w_out, preferred_element_type=jnp.float32)).astype(jnp.bfloat16)
        mem = jnp.dot(mem_out, mem_proj, preferred_element_type=jnp.float32).astype(jnp.bfloat16)
    return (jnp.stack(outputs, axis=0), mem)
```

```python
import functools
import jax
import jax.numpy as jnp
from jax import lax
from jax.experimental import pallas as pl
from jax.experimental.pallas import tpu as pltpu
from jax.sharding import PartitionSpec as P

HD = 256
F32 = jnp.float32
BF = jnp.bfloat16
NEG = -1e30


def rms_norm(rows, gain):
    values = rows.astype(F32)
    scaled = values * lax.rsqrt(jnp.mean(values * values, axis=-1, keepdims=True) + 1e-06)
    return (scaled * gain.astype(F32)).astype(BF)


def dot_t(a, b):
    return lax.dot_general(a, b, (((1,), (1,)), ((), ())), preferred_element_type=F32)


def exchange_kernel(axis, n, scatter, x_ref, o_ref, send_sem, recv_sem):
    me = lax.axis_index(axis)
    barrier = pltpu.get_barrier_semaphore()
    for d in range(1, n):
        pl.semaphore_signal(
            barrier,
            inc=1,
            device_id={axis: lax.rem(me + d, n)},
            device_id_type=pl.DeviceIdType.MESH,
        )
    pl.semaphore_wait(barrier, n - 1)
    copies = []
    for d in range(1, n):
        peer = lax.rem(me + d, n)
        copy = pltpu.make_async_remote_copy(
            src_ref=x_ref.at[peer] if scatter else x_ref,
            dst_ref=o_ref.at[me],
            send_sem=send_sem.at[d - 1],
            recv_sem=recv_sem.at[d - 1],
            device_id={axis: peer},
            device_id_type=pl.DeviceIdType.MESH,
        )
        copy.start()
        copies.append(copy)
    o_ref[me] = x_ref[me] if scatter else x_ref[...]
    for copy in copies:
        copy.wait()


def exchange(x, axis, n, ident, scatter=False):
    block = x.shape[1:] if scatter else x.shape
    vmem = pl.BlockSpec(memory_space=pltpu.VMEM)
    return pl.pallas_call(
        functools.partial(exchange_kernel, axis, n, scatter),
        out_shape=jax.ShapeDtypeStruct((n,) + block, x.dtype),
        in_specs=[vmem],
        out_specs=vmem,
        scratch_shapes=[
            pltpu.SemaphoreType.DMA((n - 1,)),
            pltpu.SemaphoreType.DMA((n - 1,)),
        ],
        compiler_params=pltpu.CompilerParams(collective_id=ident, has_side_effects=True),
        cost_estimate=pl.CostEstimate(flops=10_000_000_000, bytes_accessed=0, transcendentals=0),
    )(x)


def token_kernel(n_blocks, q_ref, qd_ref, kd_ref, mk_ref, mv_ref, *refs):
    key_refs, value_refs, o_ref = refs[:n_blocks], refs[n_blocks : 2 * n_blocks], refs[-1]
    scale = F32(HD ** (-0.5))
    rows = q_ref.shape[0]
    q_docs = qd_ref[...]
    masks = []
    for i in range(n_blocks):
        ok = q_docs == kd_ref[:, i * rows : (i + 1) * rows]
        if i == n_blocks - 1:
            row = lax.broadcasted_iota(jnp.int32, (rows, rows), 0)
            col = lax.broadcasted_iota(jnp.int32, (rows, rows), 1)
            ok = ok & (col <= row)
        masks.append(ok)
    for h in range(2):
        query = q_ref[:, h * HD : (h + 1) * HD]
        scores = [dot_t(query, mk_ref[...]) * scale]
        for i in range(n_blocks):
            scores.append(jnp.where(masks[i], dot_t(query, key_refs[i][...]) * scale, NEG))
        peak = functools.reduce(
            jnp.maximum, [jnp.max(s, axis=-1, keepdims=True) for s in scores]
        )
        total = 0.0
        mixed = 0.0
        for s, v_ref in zip(scores, (mv_ref,) + tuple(value_refs)):
            w = jnp.exp(s - peak)
            total = total + jnp.sum(w, axis=-1, keepdims=True)
            mixed = mixed + jnp.dot(w.astype(BF), v_ref[...], preferred_element_type=F32)
        o_ref[:, h * HD : (h + 1) * HD] = (mixed / total).astype(BF)


def token_attention(query, q_docs, k_docs, mem_k, mem_v, keys, values):
    rows = query.shape[0]
    groups = mem_k.shape[1] // HD
    n_blocks = len(keys)
    m = mem_k.shape[0]
    pair = pl.BlockSpec((rows, 2 * HD), lambda g: (0, g))
    one = pl.BlockSpec((rows, HD), lambda g: (0, g))
    mem = pl.BlockSpec((m, HD), lambda g: (0, g))
    return pl.pallas_call(
        functools.partial(token_kernel, n_blocks),
        grid=(groups,),
        out_shape=jax.ShapeDtypeStruct(query.shape, BF),
        in_specs=[
            pair,
            pl.BlockSpec(q_docs.shape, lambda g: (0, 0)),
            pl.BlockSpec(k_docs.shape, lambda g: (0, 0)),
            mem,
            mem,
        ]
        + [one] * n_blocks
        + [pl.BlockSpec((rows, HD), lambda g: (0, groups + g))] * n_blocks,
        out_specs=pair,
        compiler_params=pltpu.CompilerParams(vmem_limit_bytes=32 * 1024 * 1024),
        cost_estimate=pl.CostEstimate(
            flops=8 * rows * rows * n_blocks * HD * groups,
            bytes_accessed=0,
            transcendentals=0,
        ),
    )(query, q_docs, k_docs, mem_k, mem_v, *keys, *values)


def memory_kernel(groups, mq_ref, mk_ref, mv_ref, kv_ref, o_ref):
    scale = F32(HD ** (-0.5))
    first = lax.axis_index("seq") == 0
    m = mq_ref.shape[0]
    lane = lax.broadcasted_iota(jnp.int32, (m, 128), 1)
    stats = jnp.zeros((m, 128), F32)
    heads = 2 * groups
    for h in range(heads):
        g = h // 2
        query = mq_ref[:, h * HD : (h + 1) * HD]
        own = dot_t(query, mk_ref[:, g * HD : (g + 1) * HD]) * scale
        own = jnp.where(first, own, NEG)
        tok = dot_t(query, kv_ref[:, g * HD : (g + 1) * HD]) * scale
        peak = jnp.maximum(
            jnp.max(own, axis=-1, keepdims=True), jnp.max(tok, axis=-1, keepdims=True)
        )
        wo = jnp.exp(own - peak)
        wt = jnp.exp(tok - peak)
        total = jnp.sum(wo, axis=-1, keepdims=True) + jnp.sum(wt, axis=-1, keepdims=True)
        v0 = (groups + g) * HD
        mixed = jnp.dot(
            wo.astype(BF), mv_ref[:, g * HD : (g + 1) * HD], preferred_element_type=F32
        ) + jnp.dot(wt.astype(BF), kv_ref[:, v0 : v0 + HD], preferred_element_type=F32)
        o_ref[:, h * HD : (h + 1) * HD] = mixed
        stats = jnp.where(lane == h, peak, stats)
        stats = jnp.where(lane == heads + h, total, stats)
    o_ref[:, heads * HD :] = stats


def memory_partial(mem_q, mem_k, mem_v, kv):
    m, width = mem_q.shape
    groups = mem_k.shape[1] // HD
    vmem = pl.BlockSpec(memory_space=pltpu.VMEM)
    return pl.pallas_call(
        functools.partial(memory_kernel, groups),
        out_shape=jax.ShapeDtypeStruct((m, width + 128), F32),
        in_specs=[vmem] * 4,
        out_specs=vmem,
        cost_estimate=pl.CostEstimate(
            flops=8 * m * kv.shape[0] * HD * groups, bytes_accessed=0, transcendentals=0
        ),
    )(mem_q, mem_k, mem_v, kv)


def merge(parts, heads):
    n, r, _ = parts.shape
    width = heads * HD
    peaks = parts[:, :, width : width + heads]
    totals = parts[:, :, width + heads : width + 2 * heads]
    factor = jnp.exp(peaks - jnp.max(peaks, axis=0, keepdims=True))
    total = jnp.sum(totals * factor, axis=0)
    mixed = parts[:, :, :width].reshape(n, r, heads, HD) * factor[..., None]
    return (jnp.sum(mixed, axis=0) / total[..., None]).reshape(r, width)


def window(kv, n, back):
    if n % 2 or back % 2:
        return [
            lax.ppermute(kv, "seq", [(i, i + d) for i in range(n - d)])
            for d in range(1, back + 1)
        ]
    even = lax.axis_index("seq") % 2 == 0
    strides = [kv]
    for d in range(2, back + 1, 2):
        strides.append(lax.ppermute(kv, "seq", [(i, i + d) for i in range(n - d)]))
    swap = [(i, i ^ 1) for i in range(n)]
    blocks = []
    for j in range(1, len(strides)):
        blocks.append(lax.ppermute(jnp.where(even, strides[j - 1], strides[j]), "seq", swap))
        blocks.append(strides[j])
    return blocks


def per_device(
    n_seq, n_head, segment_input, doc_ids, memory, gain, w_query, w_key, w_value, w_out, mem_proj
):
    segs, rows, feat = segment_input.shape
    columns = w_out.shape[1]
    heads = w_query.shape[1] // HD
    m = memory.shape[0]
    share = m // n_seq
    longest = doc_ids.shape[1] // 2
    back = min(n_seq - 1, -(-(longest - 1) // rows))
    seq_at = lax.axis_index("seq")
    col_start = lax.axis_index("head") * columns
    row_start = seq_at * rows

    normed = rms_norm(segment_input.reshape(segs * rows, feat), gain)
    kv = jnp.concatenate(
        [
            jnp.dot(normed, w_key, preferred_element_type=F32).astype(BF),
            jnp.dot(normed, w_value, preferred_element_type=F32).astype(BF),
        ],
        axis=1,
    ).reshape(segs, rows, -1)
    query = jnp.dot(normed, w_query, preferred_element_type=F32).astype(BF)
    query = query.reshape(segs, rows, -1)
    windows = [window(kv[s], n_seq, back) for s in range(segs)]

    mem = memory
    outputs = []
    ident = 0
    for s in range(segs):
        docs = jnp.pad(doc_ids[s], (back * rows, 0), constant_values=-1)
        k_docs = lax.dynamic_slice_in_dim(docs, row_start, (back + 1) * rows, 0)
        q_docs = k_docs[back * rows :]
        normed_m = rms_norm(mem, gain)
        mem_q = jnp.dot(normed_m, w_query, preferred_element_type=F32).astype(BF)
        mem_k = jnp.dot(normed_m, w_key, preferred_element_type=F32).astype(BF)
        mem_v = jnp.dot(normed_m, w_value, preferred_element_type=F32).astype(BF)

        part = memory_partial(mem_q, mem_k, mem_v, kv[s])
        parts = exchange(part.reshape(n_seq, share, -1), "seq", n_seq, ident, scatter=True)
        attn_mem = exchange(merge(parts, heads), "head", n_head, ident + 1)
        attn_mem = attn_mem.transpose(1, 0, 2).reshape(share, -1).astype(BF)
        out_mem = jnp.dot(attn_mem, w_out, preferred_element_type=F32)
        own = lax.dynamic_slice(mem, (seq_at * share, col_start), (share, columns))
        mem_out = (own.astype(F32) + out_mem).astype(BF)
        partial_mem = jnp.dot(mem_out, mem_proj, preferred_element_type=F32)
        summed = jnp.sum(exchange(partial_mem, "head", n_head, ident + 2), axis=0)
        mem_next = exchange(summed.astype(BF).astype(F32), "seq", n_seq, ident + 3)
        ident += 4

        blocks = windows[s][::-1] + [kv[s]]
        attn_tok = token_attention(
            query[s], q_docs[:, None], k_docs[None, :], mem_k, mem_v, blocks, blocks
        )
        out_tok = jnp.dot(
            lax.all_gather(attn_tok, "head", axis=1, tiled=True),
            w_out,
            preferred_element_type=F32,
        )
        token_cols = lax.dynamic_slice_in_dim(segment_input[s], col_start, columns, 1)
        outputs.append((token_cols.astype(F32) + out_tok).astype(BF))
        mem = mem_next.reshape(m, feat).astype(BF)
    return (jnp.stack(outputs, axis=0), mem)


def solution(mesh):
    return jax.shard_map(
        functools.partial(per_device, mesh.shape["seq"], mesh.shape["head"]),
        mesh=mesh,
        in_specs=(
            P(None, "seq", None),
            P(),
            P(),
            P(),
            P(None, "head"),
            P(None, "head"),
            P(None, "head"),
            P(None, "head"),
            P("head", None),
        ),
        out_specs=(P(None, "seq", "head"), P()),
        check_vma=False,
    )
```

```python
import functools
import jax
import jax.numpy as jnp
from jax import lax
from jax.experimental import pallas as pl
from jax.experimental.pallas import tpu as pltpu
from jax.sharding import PartitionSpec as P

HD = 256
F32 = jnp.float32
BF = jnp.bfloat16
NEG = -1e30


def rms_norm(rows, gain):
    values = rows.astype(F32)
    scaled = values * lax.rsqrt(jnp.mean(values * values, axis=-1, keepdims=True) + 1e-06)
    return (scaled * gain.astype(F32)).astype(BF)


def dot_t(a, b):
    return lax.dot_general(a, b, (((1,), (1,)), ((), ())), preferred_element_type=F32)


def greet(sizes):
    barrier = pltpu.get_barrier_semaphore()
    for axis, n in sizes:
        for d in range(1, n):
            pl.semaphore_signal(
                barrier,
                inc=1,
                device_id={axis: lax.rem(lax.axis_index(axis) + d, n)},
                device_id_type=pl.DeviceIdType.MESH,
            )
    pl.semaphore_wait(barrier, sum(n - 1 for _, n in sizes))


def send_all(axis, n, source, target, send_sem, recv_sem):
    me = lax.axis_index(axis)
    copies = []
    for d in range(1, n):
        peer = lax.rem(me + d, n)
        copy = pltpu.make_async_remote_copy(
            src_ref=source(peer),
            dst_ref=target.at[me],
            send_sem=send_sem.at[d - 1],
            recv_sem=recv_sem.at[d - 1],
            device_id={axis: peer},
            device_id_type=pl.DeviceIdType.MESH,
        )
        copy.start()
        copies.append(copy)
    return copies


def merge_kernel(n_seq, n_head, heads, x_ref, o_ref, land, mine, *sems):
    me = lax.axis_index("seq")
    greet((("seq", n_seq), ("head", n_head)))
    copies = send_all("seq", n_seq, lambda peer: x_ref.at[peer], land, *sems[:2])
    land[me] = x_ref[me]
    for copy in copies:
        copy.wait()
    width = heads * HD
    stats = land[:, :, width:]
    for h in range(heads):
        peaks = stats[:, :, h : h + 1]
        factor = jnp.exp(peaks - jnp.max(peaks, axis=0, keepdims=True))
        total = jnp.sum(stats[:, :, heads + h : heads + h + 1] * factor, axis=0)
        mixed = jnp.sum(land[:, :, h * HD : (h + 1) * HD] * factor, axis=0)
        mine[:, h * HD : (h + 1) * HD] = mixed / total
    copies = send_all("head", n_head, lambda peer: mine, o_ref, *sems[2:])
    o_ref[lax.axis_index("head")] = mine[...]
    for copy in copies:
        copy.wait()


def reduce_kernel(n_seq, n_head, x_ref, o_ref, land, mine, *sems):
    greet((("seq", n_seq), ("head", n_head)))
    copies = send_all("head", n_head, lambda peer: x_ref, land, *sems[2:])
    land[lax.axis_index("head")] = x_ref[...]
    for copy in copies:
        copy.wait()
    mine[...] = jnp.sum(land[...].astype(F32), axis=0).astype(mine.dtype)
    copies = send_all("seq", n_seq, lambda peer: mine, o_ref, *sems[:2])
    o_ref[lax.axis_index("seq")] = mine[...]
    for copy in copies:
        copy.wait()


def exchange_call(kernel, x, n_seq, n_head, ident, out, land, mine):
    vmem = pl.BlockSpec(memory_space=pltpu.VMEM)
    dma = pltpu.SemaphoreType.DMA
    return pl.pallas_call(
        kernel,
        out_shape=jax.ShapeDtypeStruct(out, x.dtype),
        in_specs=[vmem],
        out_specs=vmem,
        scratch_shapes=[
            pltpu.VMEM(land, x.dtype),
            pltpu.VMEM(mine, x.dtype),
            dma((n_seq - 1,)),
            dma((n_seq - 1,)),
            dma((n_head - 1,)),
            dma((n_head - 1,)),
        ],
        compiler_params=pltpu.CompilerParams(collective_id=ident, has_side_effects=True),
        cost_estimate=pl.CostEstimate(flops=10_000_000_000, bytes_accessed=0, transcendentals=0),
    )(x)


def merge(x, n_seq, n_head, heads, ident):
    mine = (x.shape[1], heads * HD)
    return exchange_call(
        functools.partial(merge_kernel, n_seq, n_head, heads),
        x, n_seq, n_head, ident, (n_head,) + mine, x.shape, mine,
    )


def reduce(x, n_seq, n_head, ident):
    return exchange_call(
        functools.partial(reduce_kernel, n_seq, n_head),
        x, n_seq, n_head, ident, (n_seq,) + x.shape, (n_head,) + x.shape, x.shape,
    )


def after(value, *others):
    return lax.optimization_barrier((value,) + others)[0]


def token_kernel(n_blocks, q_ref, qd_ref, kd_ref, mk_ref, mv_ref, *refs):
    key_refs, value_refs, o_ref = refs[:n_blocks], refs[n_blocks : 2 * n_blocks], refs[-1]
    scale = F32(HD ** (-0.5))
    rows = q_ref.shape[0]
    q_docs = qd_ref[...]
    masks = []
    for i in range(n_blocks):
        ok = q_docs == kd_ref[:, i * rows : (i + 1) * rows]
        if i == n_blocks - 1:
            row = lax.broadcasted_iota(jnp.int32, (rows, rows), 0)
            col = lax.broadcasted_iota(jnp.int32, (rows, rows), 1)
            ok = ok & (col <= row)
        masks.append(ok)
    for h in range(2):
        query = q_ref[:, h * HD : (h + 1) * HD]
        scores = [dot_t(query, mk_ref[...]) * scale]
        for i in range(n_blocks):
            scores.append(jnp.where(masks[i], dot_t(query, key_refs[i][...]) * scale, NEG))
        peak = functools.reduce(
            jnp.maximum, [jnp.max(s, axis=-1, keepdims=True) for s in scores]
        )
        total = 0.0
        mixed = 0.0
        for s, v_ref in zip(scores, (mv_ref,) + tuple(value_refs)):
            w = jnp.exp(s - peak)
            total = total + jnp.sum(w, axis=-1, keepdims=True)
            mixed = mixed + jnp.dot(w.astype(BF), v_ref[...], preferred_element_type=F32)
        o_ref[:, h * HD : (h + 1) * HD] = (mixed / total).astype(BF)


def token_attention(query, q_docs, k_docs, mem_k, mem_v, keys, values):
    rows = query.shape[0]
    groups = mem_k.shape[1] // HD
    n_blocks = len(keys)
    m = mem_k.shape[0]
    pair = pl.BlockSpec((rows, 2 * HD), lambda g: (0, g))
    one = pl.BlockSpec((rows, HD), lambda g: (0, g))
    mem = pl.BlockSpec((m, HD), lambda g: (0, g))
    return pl.pallas_call(
        functools.partial(token_kernel, n_blocks),
        grid=(groups,),
        out_shape=jax.ShapeDtypeStruct(query.shape, BF),
        in_specs=[
            pair,
            pl.BlockSpec(q_docs.shape, lambda g: (0, 0)),
            pl.BlockSpec(k_docs.shape, lambda g: (0, 0)),
            mem,
            mem,
        ]
        + [one] * n_blocks
        + [pl.BlockSpec((rows, HD), lambda g: (0, groups + g))] * n_blocks,
        out_specs=pair,
        compiler_params=pltpu.CompilerParams(vmem_limit_bytes=32 * 1024 * 1024),
        cost_estimate=pl.CostEstimate(
            flops=8 * rows * rows * n_blocks * HD * groups,
            bytes_accessed=0,
            transcendentals=0,
        ),
    )(query, q_docs, k_docs, mem_k, mem_v, *keys, *values)


def memory_kernel(groups, mq_ref, mk_ref, mv_ref, kv_ref, o_ref):
    scale = F32(HD ** (-0.5))
    first = lax.axis_index("seq") == 0
    m = mq_ref.shape[0]
    lane = lax.broadcasted_iota(jnp.int32, (m, 128), 1)
    stats = jnp.zeros((m, 128), F32)
    heads = 2 * groups
    for h in range(heads):
        g = h // 2
        query = mq_ref[:, h * HD : (h + 1) * HD]
        own = dot_t(query, mk_ref[:, g * HD : (g + 1) * HD]) * scale
        own = jnp.where(first, own, NEG)
        tok = dot_t(query, kv_ref[:, g * HD : (g + 1) * HD]) * scale
        peak = jnp.maximum(
            jnp.max(own, axis=-1, keepdims=True), jnp.max(tok, axis=-1, keepdims=True)
        )
        wo = jnp.exp(own - peak)
        wt = jnp.exp(tok - peak)
        total = jnp.sum(wo, axis=-1, keepdims=True) + jnp.sum(wt, axis=-1, keepdims=True)
        v0 = (groups + g) * HD
        mixed = jnp.dot(
            wo.astype(BF), mv_ref[:, g * HD : (g + 1) * HD], preferred_element_type=F32
        ) + jnp.dot(wt.astype(BF), kv_ref[:, v0 : v0 + HD], preferred_element_type=F32)
        o_ref[:, h * HD : (h + 1) * HD] = mixed
        stats = jnp.where(lane == h, peak, stats)
        stats = jnp.where(lane == heads + h, total, stats)
    o_ref[:, heads * HD :] = stats


def memory_partial(mem_q, mem_k, mem_v, kv):
    m, width = mem_q.shape
    groups = mem_k.shape[1] // HD
    vmem = pl.BlockSpec(memory_space=pltpu.VMEM)
    return pl.pallas_call(
        functools.partial(memory_kernel, groups),
        out_shape=jax.ShapeDtypeStruct((m, width + 128), F32),
        in_specs=[vmem] * 4,
        out_specs=vmem,
        cost_estimate=pl.CostEstimate(
            flops=8 * m * kv.shape[0] * HD * groups, bytes_accessed=0, transcendentals=0
        ),
    )(mem_q, mem_k, mem_v, kv)


def strides_of(kv, n, back):
    step = 1 if n % 2 or back % 2 else 2
    return [kv] + [
        lax.ppermute(kv, "seq", [(i, i + d) for i in range(n - d)])
        for d in range(step, back + 1, step)
    ]


def window(strides, n, back):
    if n % 2 or back % 2:
        return strides[1:]
    even = lax.axis_index("seq") % 2 == 0
    swap = [(i, i ^ 1) for i in range(n)]
    blocks = []
    for j in range(1, len(strides)):
        blocks.append(lax.ppermute(jnp.where(even, strides[j - 1], strides[j]), "seq", swap))
        blocks.append(strides[j])
    return blocks


def per_device(
    n_seq, n_head, segment_input, doc_ids, memory, gain, w_query, w_key, w_value, w_out, mem_proj
):
    segs, rows, feat = segment_input.shape
    columns = w_out.shape[1]
    heads = w_query.shape[1] // HD
    m = memory.shape[0]
    share = m // n_seq
    longest = doc_ids.shape[1] // 2
    back = min(n_seq - 1, -(-(longest - 1) // rows))
    seq_at = lax.axis_index("seq")
    col_start = lax.axis_index("head") * columns
    row_start = seq_at * rows

    normed = rms_norm(segment_input.reshape(segs * rows, feat), gain)
    kv = jnp.concatenate(
        [
            jnp.dot(normed, w_key, preferred_element_type=F32).astype(BF),
            jnp.dot(normed, w_value, preferred_element_type=F32).astype(BF),
        ],
        axis=1,
    ).reshape(segs, rows, -1)
    query = jnp.dot(normed, w_query, preferred_element_type=F32).astype(BF)
    query = query.reshape(segs, rows, -1)
    strides = strides_of(kv[0], n_seq, back)

    mem = memory
    outputs = []
    for s in range(segs):
        docs = jnp.pad(doc_ids[s], (back * rows, 0), constant_values=-1)
        k_docs = lax.dynamic_slice_in_dim(docs, row_start, (back + 1) * rows, 0)
        q_docs = k_docs[back * rows :]
        normed_m = rms_norm(mem, gain)
        mem_q = jnp.dot(normed_m, w_query, preferred_element_type=F32).astype(BF)
        mem_k = jnp.dot(normed_m, w_key, preferred_element_type=F32).astype(BF)
        mem_v = jnp.dot(normed_m, w_value, preferred_element_type=F32).astype(BF)

        part = memory_partial(mem_q, mem_k, mem_v, kv[s])
        blocks = window(strides, n_seq, back)[::-1] + [kv[s]]
        attn_tok = token_attention(
            query[s], q_docs[:, None], k_docs[None, :], mem_k, mem_v, blocks, blocks
        )
        gathered = lax.all_gather(attn_tok, "head", axis=1, tiled=True)

        part = after(part, attn_tok)
        attn_mem = merge(part.reshape(n_seq, share, -1), n_seq, n_head, heads, 2 * s)
        if s + 1 < segs:
            strides = strides_of(after(kv[s + 1], attn_mem), n_seq, back)
        attn_mem = attn_mem.transpose(1, 0, 2).reshape(share, -1).astype(BF)
        out_mem = jnp.dot(attn_mem, w_out, preferred_element_type=F32)
        own = lax.dynamic_slice(mem, (seq_at * share, col_start), (share, columns))
        mem_out = (own.astype(F32) + out_mem).astype(BF)
        partial_mem = jnp.dot(mem_out, mem_proj, preferred_element_type=F32).astype(BF)
        mem_next = reduce(partial_mem, n_seq, n_head, 2 * s + 1)

        token_cols = lax.dynamic_slice_in_dim(segment_input[s], col_start, columns, 1)
        out_tok = jnp.dot(gathered, w_out, preferred_element_type=F32)
        outputs.append((token_cols.astype(F32) + out_tok).astype(BF))
        mem = mem_next.reshape(m, feat)
    return (jnp.stack(outputs, axis=0), mem)


def solution(mesh):
    return jax.shard_map(
        functools.partial(per_device, mesh.shape["seq"], mesh.shape["head"]),
        mesh=mesh,
        in_specs=(
            P(None, "seq", None),
            P(),
            P(),
            P(),
            P(None, "head"),
            P(None, "head"),
            P(None, "head"),
            P(None, "head"),
            P("head", None),
        ),
        out_specs=(P(None, "seq", "head"), P()),
        check_vma=False,
    )
```

```python
import functools
import jax
import jax.numpy as jnp
from jax import lax
from jax.experimental import pallas as pl
from jax.experimental.pallas import tpu as pltpu
from jax.sharding import PartitionSpec as P

HD = 256
F32 = jnp.float32
BF = jnp.bfloat16
NEG = -1e30


def rms_norm(rows, gain):
    values = rows.astype(F32)
    scaled = values * lax.rsqrt(jnp.mean(values * values, axis=-1, keepdims=True) + 1e-06)
    return (scaled * gain.astype(F32)).astype(BF)


def dot_t(a, b):
    return lax.dot_general(a, b, (((1,), (1,)), ((), ())), preferred_element_type=F32)


def greet(sizes):
    barrier = pltpu.get_barrier_semaphore()
    for axis, n in sizes:
        for d in range(1, n):
            pl.semaphore_signal(
                barrier,
                inc=1,
                device_id={axis: lax.rem(lax.axis_index(axis) + d, n)},
                device_id_type=pl.DeviceIdType.MESH,
            )
    pl.semaphore_wait(barrier, sum(n - 1 for _, n in sizes))


def send_all(axis, n, source, target, send_sem, recv_sem):
    me = lax.axis_index(axis)
    copies = []
    for d in range(1, n):
        peer = lax.rem(me + d, n)
        copy = pltpu.make_async_remote_copy(
            src_ref=source(peer),
            dst_ref=target.at[me],
            send_sem=send_sem.at[d - 1],
            recv_sem=recv_sem.at[d - 1],
            device_id={axis: peer},
            device_id_type=pl.DeviceIdType.MESH,
        )
        copy.start()
        copies.append(copy)
    return copies


def merge_kernel(n_seq, n_head, heads, x_ref, o_ref, land, mine, *sems):
    me = lax.axis_index("seq")
    greet((("seq", n_seq), ("head", n_head)))
    copies = send_all("seq", n_seq, lambda peer: x_ref.at[peer], land, *sems[:2])
    land[me] = x_ref[me]
    for copy in copies:
        copy.wait()
    width = heads * HD
    stats = land[:, :, width:]
    for h in range(heads):
        peaks = stats[:, :, h : h + 1]
        factor = jnp.exp(peaks - jnp.max(peaks, axis=0, keepdims=True))
        total = jnp.sum(stats[:, :, heads + h : heads + h + 1] * factor, axis=0)
        mixed = jnp.sum(land[:, :, h * HD : (h + 1) * HD] * factor, axis=0)
        mine[:, h * HD : (h + 1) * HD] = mixed / total
    copies = send_all("head", n_head, lambda peer: mine, o_ref, *sems[2:])
    o_ref[lax.axis_index("head")] = mine[...]
    for copy in copies:
        copy.wait()


def reduce_kernel(n_seq, n_head, x_ref, o_ref, land, mine, *sems):
    greet((("seq", n_seq), ("head", n_head)))
    copies = send_all("head", n_head, lambda peer: x_ref, land, *sems[2:])
    land[lax.axis_index("head")] = x_ref[...]
    for copy in copies:
        copy.wait()
    mine[...] = jnp.sum(land[...].astype(F32), axis=0).astype(mine.dtype)
    copies = send_all("seq", n_seq, lambda peer: mine, o_ref, *sems[:2])
    o_ref[lax.axis_index("seq")] = mine[...]
    for copy in copies:
        copy.wait()


def exchange_call(kernel, x, n_seq, n_head, ident, out, land, mine):
    vmem = pl.BlockSpec(memory_space=pltpu.VMEM)
    dma = pltpu.SemaphoreType.DMA
    return pl.pallas_call(
        kernel,
        out_shape=jax.ShapeDtypeStruct(out, x.dtype),
        in_specs=[vmem],
        out_specs=vmem,
        scratch_shapes=[
            pltpu.VMEM(land, x.dtype),
            pltpu.VMEM(mine, x.dtype),
            dma((n_seq - 1,)),
            dma((n_seq - 1,)),
            dma((n_head - 1,)),
            dma((n_head - 1,)),
        ],
        compiler_params=pltpu.CompilerParams(collective_id=ident, has_side_effects=True),
        cost_estimate=pl.CostEstimate(flops=1_000_000_000, bytes_accessed=0, transcendentals=0),
    )(x)


def merge(x, n_seq, n_head, heads, ident):
    mine = (x.shape[1], heads * HD)
    return exchange_call(
        functools.partial(merge_kernel, n_seq, n_head, heads),
        x, n_seq, n_head, ident, (n_head,) + mine, x.shape, mine,
    )


def reduce(x, n_seq, n_head, ident):
    return exchange_call(
        functools.partial(reduce_kernel, n_seq, n_head),
        x, n_seq, n_head, ident, (n_seq,) + x.shape, (n_head,) + x.shape, x.shape,
    )


def after(value, *others):
    return lax.optimization_barrier((value,) + others)[0]


def token_kernel(n_blocks, q_ref, qd_ref, kd_ref, mk_ref, mv_ref, *refs):
    key_refs, value_refs, o_ref = refs[:n_blocks], refs[n_blocks : 2 * n_blocks], refs[-1]
    scale = F32(HD ** (-0.5))
    rows = q_ref.shape[0]
    q_docs = qd_ref[...]
    masks = []
    for i in range(n_blocks):
        ok = q_docs == kd_ref[:, i * rows : (i + 1) * rows]
        if i == n_blocks - 1:
            row = lax.broadcasted_iota(jnp.int32, (rows, rows), 0)
            col = lax.broadcasted_iota(jnp.int32, (rows, rows), 1)
            ok = ok & (col <= row)
        masks.append(ok)
    for h in range(2):
        query = q_ref[:, h * HD : (h + 1) * HD]
        scores = [dot_t(query, mk_ref[...]) * scale]
        for i in range(n_blocks):
            scores.append(jnp.where(masks[i], dot_t(query, key_refs[i][...]) * scale, NEG))
        peak = functools.reduce(
            jnp.maximum, [jnp.max(s, axis=-1, keepdims=True) for s in scores]
        )
        total = 0.0
        mixed = 0.0
        for s, v_ref in zip(scores, (mv_ref,) + tuple(value_refs)):
            w = jnp.exp(s - peak)
            total = total + jnp.sum(w, axis=-1, keepdims=True)
            mixed = mixed + jnp.dot(w.astype(BF), v_ref[...], preferred_element_type=F32)
        o_ref[:, h * HD : (h + 1) * HD] = (mixed / total).astype(BF)


def token_attention(query, q_docs, k_docs, mem_k, mem_v, keys, values):
    rows = query.shape[0]
    groups = mem_k.shape[1] // HD
    n_blocks = len(keys)
    m = mem_k.shape[0]
    pair = pl.BlockSpec((rows, 2 * HD), lambda g: (0, g))
    one = pl.BlockSpec((rows, HD), lambda g: (0, g))
    mem = pl.BlockSpec((m, HD), lambda g: (0, g))
    return pl.pallas_call(
        functools.partial(token_kernel, n_blocks),
        grid=(groups,),
        out_shape=jax.ShapeDtypeStruct(query.shape, BF),
        in_specs=[
            pair,
            pl.BlockSpec(q_docs.shape, lambda g: (0, 0)),
            pl.BlockSpec(k_docs.shape, lambda g: (0, 0)),
            mem,
            mem,
        ]
        + [one] * n_blocks
        + [pl.BlockSpec((rows, HD), lambda g: (0, groups + g))] * n_blocks,
        out_specs=pair,
        compiler_params=pltpu.CompilerParams(vmem_limit_bytes=32 * 1024 * 1024),
        cost_estimate=pl.CostEstimate(
            flops=8 * rows * rows * n_blocks * HD * groups,
            bytes_accessed=0,
            transcendentals=0,
        ),
    )(query, q_docs, k_docs, mem_k, mem_v, *keys, *values)


def memory_kernel(groups, mq_ref, mk_ref, mv_ref, kv_ref, o_ref):
    scale = F32(HD ** (-0.5))
    first = lax.axis_index("seq") == 0
    m = mq_ref.shape[0]
    lane = lax.broadcasted_iota(jnp.int32, (m, 128), 1)
    stats = jnp.zeros((m, 128), F32)
    heads = 2 * groups
    for h in range(heads):
        g = h // 2
        query = mq_ref[:, h * HD : (h + 1) * HD]
        own = dot_t(query, mk_ref[:, g * HD : (g + 1) * HD]) * scale
        own = jnp.where(first, own, NEG)
        tok = dot_t(query, kv_ref[:, g * HD : (g + 1) * HD]) * scale
        peak = jnp.maximum(
            jnp.max(own, axis=-1, keepdims=True), jnp.max(tok, axis=-1, keepdims=True)
        )
        wo = jnp.exp(own - peak)
        wt = jnp.exp(tok - peak)
        total = jnp.sum(wo, axis=-1, keepdims=True) + jnp.sum(wt, axis=-1, keepdims=True)
        v0 = (groups + g) * HD
        mixed = jnp.dot(
            wo.astype(BF), mv_ref[:, g * HD : (g + 1) * HD], preferred_element_type=F32
        ) + jnp.dot(wt.astype(BF), kv_ref[:, v0 : v0 + HD], preferred_element_type=F32)
        o_ref[:, h * HD : (h + 1) * HD] = mixed
        stats = jnp.where(lane == h, peak, stats)
        stats = jnp.where(lane == heads + h, total, stats)
    o_ref[:, heads * HD :] = stats


def memory_partial(mem_q, mem_k, mem_v, kv):
    m, width = mem_q.shape
    groups = mem_k.shape[1] // HD
    vmem = pl.BlockSpec(memory_space=pltpu.VMEM)
    return pl.pallas_call(
        functools.partial(memory_kernel, groups),
        out_shape=jax.ShapeDtypeStruct((m, width + 128), F32),
        in_specs=[vmem] * 4,
        out_specs=vmem,
        cost_estimate=pl.CostEstimate(
            flops=8 * m * kv.shape[0] * HD * groups, bytes_accessed=0, transcendentals=0
        ),
    )(mem_q, mem_k, mem_v, kv)


def strides_of(kv, n, back):
    step = 1 if n % 2 or back % 2 else 2
    return [kv] + [
        lax.ppermute(kv, "seq", [(i, i + d) for i in range(n - d)])
        for d in range(step, back + 1, step)
    ]


def window(strides, n, back):
    if n % 2 or back % 2:
        return strides[1:]
    even = lax.axis_index("seq") % 2 == 0
    swap = [(i, i ^ 1) for i in range(n)]
    blocks = []
    for j in range(1, len(strides)):
        blocks.append(lax.ppermute(jnp.where(even, strides[j - 1], strides[j]), "seq", swap))
        blocks.append(strides[j])
    return blocks


def per_device(
    n_seq, n_head, segment_input, doc_ids, memory, gain, w_query, w_key, w_value, w_out, mem_proj
):
    segs, rows, feat = segment_input.shape
    columns = w_out.shape[1]
    heads = w_query.shape[1] // HD
    m = memory.shape[0]
    share = m // n_seq
    longest = doc_ids.shape[1] // 2
    back = min(n_seq - 1, -(-(longest - 1) // rows))
    seq_at = lax.axis_index("seq")
    col_start = lax.axis_index("head") * columns
    row_start = seq_at * rows

    normed = rms_norm(segment_input.reshape(segs * rows, feat), gain)
    kv = jnp.concatenate(
        [
            jnp.dot(normed, w_key, preferred_element_type=F32).astype(BF),
            jnp.dot(normed, w_value, preferred_element_type=F32).astype(BF),
        ],
        axis=1,
    ).reshape(segs, rows, -1)
    query = jnp.dot(normed, w_query, preferred_element_type=F32).astype(BF)
    query = query.reshape(segs, rows, -1)
    strides = strides_of(kv[0], n_seq, back)

    mem = memory
    outputs = []
    for s in range(segs):
        docs = jnp.pad(doc_ids[s], (back * rows, 0), constant_values=-1)
        k_docs = lax.dynamic_slice_in_dim(docs, row_start, (back + 1) * rows, 0)
        q_docs = k_docs[back * rows :]
        normed_m = rms_norm(mem, gain)
        mem_k = jnp.dot(normed_m, w_key, preferred_element_type=F32).astype(BF)
        mem_v = jnp.dot(normed_m, w_value, preferred_element_type=F32).astype(BF)

        blocks = window(strides, n_seq, back)[::-1] + [kv[s]]
        attn_tok = token_attention(
            query[s], q_docs[:, None], k_docs[None, :], mem_k, mem_v, blocks, blocks
        )
        gathered = lax.all_gather(attn_tok, "head", axis=1, tiled=True)

        rows_m = after(normed_m, attn_tok) if s else normed_m
        mem_q = jnp.dot(rows_m, w_query, preferred_element_type=F32).astype(BF)
        part = memory_partial(mem_q, mem_k, mem_v, kv[s])
        part = after(part, attn_tok)
        attn_mem = merge(part.reshape(n_seq, share, -1), n_seq, n_head, heads, 2 * s)
        if s + 1 < segs:
            strides = strides_of(after(kv[s + 1], attn_mem), n_seq, back)
        attn_mem = attn_mem.transpose(1, 0, 2).reshape(share, -1).astype(BF)
        out_mem = jnp.dot(attn_mem, w_out, preferred_element_type=F32)
        own = lax.dynamic_slice(mem, (seq_at * share, col_start), (share, columns))
        mem_out = (own.astype(F32) + out_mem).astype(BF)
        partial_mem = jnp.dot(mem_out, mem_proj, preferred_element_type=F32).astype(BF)
        mem_next = reduce(partial_mem, n_seq, n_head, 2 * s + 1)

        token_cols = lax.dynamic_slice(
            segment_input, (s, 0, col_start), (1, rows, columns)
        ).reshape(rows, columns)
        out_tok = jnp.dot(gathered, w_out, preferred_element_type=F32)
        outputs.append((token_cols.astype(F32) + out_tok).astype(BF))
        mem = mem_next.reshape(m, feat)
    return (jnp.stack(outputs, axis=0), mem)


def solution(mesh):
    return jax.shard_map(
        functools.partial(per_device, mesh.shape["seq"], mesh.shape["head"]),
        mesh=mesh,
        in_specs=(
            P(None, "seq", None),
            P(),
            P(),
            P(),
            P(None, "head"),
            P(None, "head"),
            P(None, "head"),
            P(None, "head"),
            P("head", None),
        ),
        out_specs=(P(None, "seq", "head"), P()),
        check_vma=False,
    )
```

```python
import functools
import jax
import jax.numpy as jnp
from jax import lax
from jax.experimental import pallas as pl
from jax.experimental.pallas import tpu as pltpu
from jax.sharding import PartitionSpec as P

HD = 256
F32 = jnp.float32
BF = jnp.bfloat16
NEG = -1e30


def rms_norm(rows, gain):
    values = rows.astype(F32)
    scaled = values * lax.rsqrt(jnp.mean(values * values, axis=-1, keepdims=True) + 1e-06)
    return (scaled * gain.astype(F32)).astype(BF)


def dot_t(a, b):
    return lax.dot_general(a, b, (((1,), (1,)), ((), ())), preferred_element_type=F32)


def greet(sizes):
    barrier = pltpu.get_barrier_semaphore()
    for axis, n in sizes:
        for d in range(1, n):
            pl.semaphore_signal(
                barrier,
                inc=1,
                device_id={axis: lax.rem(lax.axis_index(axis) + d, n)},
                device_id_type=pl.DeviceIdType.MESH,
            )
    pl.semaphore_wait(barrier, sum(n - 1 for _, n in sizes))


def send_all(axis, n, source, target, send_sem, recv_sem):
    me = lax.axis_index(axis)
    copies = []
    for d in range(1, n):
        peer = lax.rem(me + d, n)
        copy = pltpu.make_async_remote_copy(
            src_ref=source(peer),
            dst_ref=target.at[me],
            send_sem=send_sem.at[d - 1],
            recv_sem=recv_sem.at[d - 1],
            device_id={axis: peer},
            device_id_type=pl.DeviceIdType.MESH,
        )
        copy.start()
        copies.append(copy)
    return copies


def merge_kernel(n_seq, n_head, heads, x_ref, o_ref, land, mine, *sems):
    me = lax.axis_index("seq")
    greet((("seq", n_seq), ("head", n_head)))
    copies = send_all("seq", n_seq, lambda peer: x_ref.at[peer], land, *sems[:2])
    land[me] = x_ref[me]
    for copy in copies:
        copy.wait()
    width = heads * HD
    stats = land[:, :, width:]
    for h in range(heads):
        peaks = stats[:, :, h : h + 1]
        factor = jnp.exp(peaks - jnp.max(peaks, axis=0, keepdims=True))
        total = jnp.sum(stats[:, :, heads + h : heads + h + 1] * factor, axis=0)
        mixed = jnp.sum(land[:, :, h * HD : (h + 1) * HD] * factor, axis=0)
        mine[:, h * HD : (h + 1) * HD] = mixed / total
    copies = send_all("head", n_head, lambda peer: mine, o_ref, *sems[2:])
    o_ref[lax.axis_index("head")] = mine[...]
    for copy in copies:
        copy.wait()


def reduce_kernel(n_seq, n_head, x_ref, o_ref, land, mine, *sems):
    greet((("seq", n_seq), ("head", n_head)))
    copies = send_all("head", n_head, lambda peer: x_ref, land, *sems[2:])
    land[lax.axis_index("head")] = x_ref[...]
    for copy in copies:
        copy.wait()
    mine[...] = jnp.sum(land[...].astype(F32), axis=0).astype(mine.dtype)
    copies = send_all("seq", n_seq, lambda peer: mine, o_ref, *sems[:2])
    o_ref[lax.axis_index("seq")] = mine[...]
    for copy in copies:
        copy.wait()


def exchange_call(kernel, x, n_seq, n_head, ident, out, land, mine):
    vmem = pl.BlockSpec(memory_space=pltpu.VMEM)
    dma = pltpu.SemaphoreType.DMA
    return pl.pallas_call(
        kernel,
        out_shape=jax.ShapeDtypeStruct(out, x.dtype),
        in_specs=[vmem],
        out_specs=vmem,
        scratch_shapes=[
            pltpu.VMEM(land, x.dtype),
            pltpu.VMEM(mine, x.dtype),
            dma((n_seq - 1,)),
            dma((n_seq - 1,)),
            dma((n_head - 1,)),
            dma((n_head - 1,)),
        ],
        compiler_params=pltpu.CompilerParams(collective_id=ident, has_side_effects=True),
        cost_estimate=pl.CostEstimate(flops=1_000_000_000, bytes_accessed=0, transcendentals=0),
    )(x)


def merge(x, n_seq, n_head, heads, ident):
    mine = (x.shape[1], heads * HD)
    return exchange_call(
        functools.partial(merge_kernel, n_seq, n_head, heads),
        x, n_seq, n_head, ident, (n_head,) + mine, x.shape, mine,
    )


def reduce(x, n_seq, n_head, ident):
    return exchange_call(
        functools.partial(reduce_kernel, n_seq, n_head),
        x, n_seq, n_head, ident, (n_seq,) + x.shape, (n_head,) + x.shape, x.shape,
    )


def after(value, *others):
    return lax.optimization_barrier((value,) + others)[0]


def token_kernel(n_blocks, q_ref, qd_ref, kd_ref, mk_ref, mv_ref, *refs):
    key_refs, value_refs, o_ref = refs[:n_blocks], refs[n_blocks : 2 * n_blocks], refs[-1]
    scale = F32(HD ** (-0.5))
    rows = q_ref.shape[0]
    q_docs = qd_ref[...]
    masks = []
    for i in range(n_blocks):
        ok = q_docs == kd_ref[:, i * rows : (i + 1) * rows]
        if i == n_blocks - 1:
            row = lax.broadcasted_iota(jnp.int32, (rows, rows), 0)
            col = lax.broadcasted_iota(jnp.int32, (rows, rows), 1)
            ok = ok & (col <= row)
        masks.append(ok)
    for h in range(2):
        query = q_ref[:, h * HD : (h + 1) * HD]
        scores = [dot_t(query, mk_ref[...]) * scale]
        for i in range(n_blocks):
            scores.append(jnp.where(masks[i], dot_t(query, key_refs[i][...]) * scale, NEG))
        peak = functools.reduce(
            jnp.maximum, [jnp.max(s, axis=-1, keepdims=True) for s in scores]
        )
        total = 0.0
        mixed = 0.0
        for s, v_ref in zip(scores, (mv_ref,) + tuple(value_refs)):
            w = jnp.exp(s - peak)
            total = total + jnp.sum(w, axis=-1, keepdims=True)
            mixed = mixed + jnp.dot(w.astype(BF), v_ref[...], preferred_element_type=F32)
        o_ref[:, h * HD : (h + 1) * HD] = (mixed / total).astype(BF)


def token_attention(query, q_docs, k_docs, mem_k, mem_v, keys, values):
    rows = query.shape[0]
    groups = mem_k.shape[1] // HD
    n_blocks = len(keys)
    m = mem_k.shape[0]
    pair = pl.BlockSpec((rows, 2 * HD), lambda g: (0, g))
    one = pl.BlockSpec((rows, HD), lambda g: (0, g))
    mem = pl.BlockSpec((m, HD), lambda g: (0, g))
    return pl.pallas_call(
        functools.partial(token_kernel, n_blocks),
        grid=(groups,),
        out_shape=jax.ShapeDtypeStruct(query.shape, BF),
        in_specs=[
            pair,
            pl.BlockSpec(q_docs.shape, lambda g: (0, 0)),
            pl.BlockSpec(k_docs.shape, lambda g: (0, 0)),
            mem,
            mem,
        ]
        + [one] * n_blocks
        + [pl.BlockSpec((rows, HD), lambda g: (0, groups + g))] * n_blocks,
        out_specs=pair,
        compiler_params=pltpu.CompilerParams(vmem_limit_bytes=32 * 1024 * 1024),
        cost_estimate=pl.CostEstimate(
            flops=8 * rows * rows * n_blocks * HD * groups,
            bytes_accessed=0,
            transcendentals=0,
        ),
    )(query, q_docs, k_docs, mem_k, mem_v, *keys, *values)


def memory_kernel(groups, mq_ref, mk_ref, mv_ref, kv_ref, o_ref):
    scale = F32(HD ** (-0.5))
    first = lax.axis_index("seq") == 0
    m = mq_ref.shape[0]
    lane = lax.broadcasted_iota(jnp.int32, (m, 128), 1)
    stats = jnp.zeros((m, 128), F32)
    heads = 2 * groups
    for h in range(heads):
        g = h // 2
        query = mq_ref[:, h * HD : (h + 1) * HD]
        own = dot_t(query, mk_ref[:, g * HD : (g + 1) * HD]) * scale
        own = jnp.where(first, own, NEG)
        tok = dot_t(query, kv_ref[:, g * HD : (g + 1) * HD]) * scale
        peak = jnp.maximum(
            jnp.max(own, axis=-1, keepdims=True), jnp.max(tok, axis=-1, keepdims=True)
        )
        wo = jnp.exp(own - peak)
        wt = jnp.exp(tok - peak)
        total = jnp.sum(wo, axis=-1, keepdims=True) + jnp.sum(wt, axis=-1, keepdims=True)
        v0 = (groups + g) * HD
        mixed = jnp.dot(
            wo.astype(BF), mv_ref[:, g * HD : (g + 1) * HD], preferred_element_type=F32
        ) + jnp.dot(wt.astype(BF), kv_ref[:, v0 : v0 + HD], preferred_element_type=F32)
        o_ref[:, h * HD : (h + 1) * HD] = mixed
        stats = jnp.where(lane == h, peak, stats)
        stats = jnp.where(lane == heads + h, total, stats)
    o_ref[:, heads * HD :] = stats


def memory_partial(mem_q, mem_k, mem_v, kv):
    m, width = mem_q.shape
    groups = mem_k.shape[1] // HD
    vmem = pl.BlockSpec(memory_space=pltpu.VMEM)
    return pl.pallas_call(
        functools.partial(memory_kernel, groups),
        out_shape=jax.ShapeDtypeStruct((m, width + 128), F32),
        in_specs=[vmem] * 4,
        out_specs=vmem,
        cost_estimate=pl.CostEstimate(
            flops=8 * m * kv.shape[0] * HD * groups, bytes_accessed=0, transcendentals=0
        ),
    )(mem_q, mem_k, mem_v, kv)


def strides_of(kv, n, back):
    step = 1 if n % 2 or back % 2 else 2
    return [kv] + [
        lax.ppermute(kv, "seq", [(i, i + d) for i in range(n - d)])
        for d in range(step, back + 1, step)
    ]


def window(strides, n, back):
    if n % 2 or back % 2:
        return strides[1:]
    even = lax.axis_index("seq") % 2 == 0
    swap = [(i, i ^ 1) for i in range(n)]
    blocks = []
    for j in range(1, len(strides)):
        blocks.append(lax.ppermute(jnp.where(even, strides[j - 1], strides[j]), "seq", swap))
        blocks.append(strides[j])
    return blocks


def per_device(
    n_seq, n_head, segment_input, doc_ids, memory, gain, w_query, w_key, w_value, w_out, mem_proj
):
    segs, rows, feat = segment_input.shape
    columns = w_out.shape[1]
    heads = w_query.shape[1] // HD
    m = memory.shape[0]
    share = m // n_seq
    longest = doc_ids.shape[1] // 2
    back = min(n_seq - 1, -(-(longest - 1) // rows))
    seq_at = lax.axis_index("seq")
    col_start = lax.axis_index("head") * columns
    row_start = seq_at * rows

    normed = rms_norm(segment_input.reshape(segs * rows, feat), gain)
    kv = jnp.concatenate(
        [
            jnp.dot(normed, w_key, preferred_element_type=F32).astype(BF),
            jnp.dot(normed, w_value, preferred_element_type=F32).astype(BF),
        ],
        axis=1,
    ).reshape(segs, rows, -1)
    query = jnp.dot(normed, w_query, preferred_element_type=F32).astype(BF)
    query = query.reshape(segs, rows, -1)
    strides = strides_of(kv[0], n_seq, back)

    mem = memory
    outputs = []
    for s in range(segs):
        docs = jnp.pad(doc_ids[s], (back * rows, 0), constant_values=-1)
        k_docs = lax.dynamic_slice_in_dim(docs, row_start, (back + 1) * rows, 0)
        q_docs = k_docs[back * rows :]
        normed_m = rms_norm(mem, gain)
        mem_k = jnp.dot(normed_m, w_key, preferred_element_type=F32).astype(BF)
        mem_v = jnp.dot(normed_m, w_value, preferred_element_type=F32).astype(BF)

        blocks = window(strides, n_seq, back)[::-1] + [kv[s]]
        token_q = query[s]
        if s == 0:
            mem_q = jnp.dot(normed_m, w_query, preferred_element_type=F32).astype(BF)
            part = memory_partial(mem_q, mem_k, mem_v, kv[s])
            token_q = after(token_q, part)
        attn_tok = token_attention(
            token_q, q_docs[:, None], k_docs[None, :], mem_k, mem_v, blocks, blocks
        )
        gathered = lax.all_gather(attn_tok, "head", axis=1, tiled=True)

        if s > 0:
            rows_m = after(normed_m, attn_tok)
            mem_q = jnp.dot(rows_m, w_query, preferred_element_type=F32).astype(BF)
            part = memory_partial(mem_q, mem_k, mem_v, kv[s])
        part = after(part, attn_tok)
        attn_mem = merge(part.reshape(n_seq, share, -1), n_seq, n_head, heads, 2 * s)
        if s + 1 < segs:
            strides = strides_of(after(kv[s + 1], attn_mem), n_seq, back)
        attn_mem = attn_mem.transpose(1, 0, 2).reshape(share, -1).astype(BF)
        out_mem = jnp.dot(attn_mem, w_out, preferred_element_type=F32)
        own = lax.dynamic_slice(mem, (seq_at * share, col_start), (share, columns))
        mem_out = (own.astype(F32) + out_mem).astype(BF)
        partial_mem = jnp.dot(mem_out, mem_proj, preferred_element_type=F32).astype(BF)
        mem_next = reduce(partial_mem, n_seq, n_head, 2 * s + 1)

        token_cols = lax.dynamic_slice(
            segment_input, (s, 0, col_start), (1, rows, columns)
        ).reshape(rows, columns)
        out_tok = jnp.dot(gathered, w_out, preferred_element_type=F32)
        outputs.append((token_cols.astype(F32) + out_tok).astype(BF))
        mem = mem_next.reshape(m, feat)
    return (jnp.stack(outputs, axis=0), mem)


def solution(mesh):
    return jax.shard_map(
        functools.partial(per_device, mesh.shape["seq"], mesh.shape["head"]),
        mesh=mesh,
        in_specs=(
            P(None, "seq", None),
            P(),
            P(),
            P(),
            P(None, "head"),
            P(None, "head"),
            P(None, "head"),
            P(None, "head"),
            P("head", None),
        ),
        out_specs=(P(None, "seq", "head"), P()),
        check_vma=False,
    )
```
